8 devices in a mesh: dp: 4 (over z, y, x), ep: 2 (over core).
Axes of the slice: x: 2, y: 2, z: 1, core: 2. Of those that a mesh axis runs over, the one named last changes fastest.
Arguments:
- x_in: bfloat16 [8192, 1536], P(('dp', 'ep'))
- dy_in: bfloat16 [8192, 1536], P(('dp', 'ep'))
- top_ids: int32 [8192, 6], P(('dp', 'ep'))
- w_router: bfloat16 [1536, 64], P(('dp', 'ep'))
- w_gate: bfloat16 [64, 1536, 512], P('ep', 'dp')
- w_up: bfloat16 [64, 1536, 512], P('ep', 'dp')
- w_down: bfloat16 [64, 512, 1536], P('ep', 'dp')
- s_gate: bfloat16 [1536, 1024], P(('dp', 'ep'))
- s_up: bfloat16 [1536, 1024], P(('dp', 'ep'))
- s_down: bfloat16 [1024, 1536], P(('dp', 'ep'))
Outputs:
- output 1: bfloat16 [8192, 1536], P(('dp', 'ep'))
- output 2: bfloat16 [8192, 1536], P(('dp', 'ep'))
- output 3: float32 [1536, 64], P(('dp', 'ep'))
- output 4: float32 [64, 1536, 512], P('ep', 'dp')
- output 5: float32 [64, 1536, 512], P('ep', 'dp')
- output 6: float32 [64, 512, 1536], P('ep', 'dp')
- output 7: float32 [1536, 1024], P(('dp', 'ep'))
- output 8: float32 [1536, 1024], P(('dp', 'ep'))
- output 9: float32 [1024, 1536], P(('dp', 'ep'))
All inputs are finite; a program needn't handle non-finite values.
Results may differ from the reference program's by a relative error of at most 0.00505773.
Values are sent between devices in bfloat16 or wider.
A program may use at most 1 GiB of HBM per device.

```python
import math
import jax
import jax.numpy as jnp
from jax import lax

MODEL_DIM = 1536
NUM_EXPERTS = 64
TOP_K = 6
EXPERT_FF = 512
SHARED_FF = 1024
TOK_DEV = 1024
NUM_BLOCKS = 8
SLOT_CAP = 2 * TOK_DEV * TOP_K // NUM_EXPERTS
TOKENS = TOK_DEV * NUM_BLOCKS


def draw_routes(route_key):
    choices = TOK_DEV * TOP_K
    rank_expert = jax.random.permutation(jax.random.fold_in(route_key, 1), NUM_EXPERTS)
    rank_ids = jnp.arange(1, NUM_EXPERTS, dtype=jnp.int32)
    weights = 16384 // (rank_ids + NUM_EXPERTS // 2)
    spare_cnt = choices - SLOT_CAP - (NUM_EXPERTS - 1)
    base_cnt = 1 + (spare_cnt * weights) // jnp.sum(weights)
    short_cnt = spare_cnt - jnp.sum(base_cnt - 1)
    tail_cnt = base_cnt + (rank_ids >= NUM_EXPERTS - short_cnt).astype(jnp.int32)
    counts = jnp.concatenate([jnp.full((1,), SLOT_CAP, dtype=jnp.int32), tail_cnt])
    run_ends = jnp.cumsum(counts)
    slot_rank = jnp.searchsorted(run_ends, jnp.arange(choices, dtype=jnp.int32), side='right')
    id_grid = rank_expert[slot_rank].reshape(TOP_K, TOK_DEV).T
    blk_keys = jax.random.split(jax.random.fold_in(route_key, 2), NUM_BLOCKS)
    blocks = jax.vmap(lambda blk_key: id_grid[jax.random.permutation(blk_key, TOK_DEV)])(blk_keys)
    return blocks.reshape(TOKENS, TOP_K).astype(jnp.int32)


def setup_inputs(seed: int = 0) -> dict:
    sub_keys = jax.random.split(jax.random.key(seed), 11)
    top_ids = draw_routes(sub_keys[0])
    w_router = (jax.random.normal(sub_keys[1], (MODEL_DIM, NUM_EXPERTS), jnp.float32) * MODEL_DIM ** -0.5).astype(jnp.bfloat16)
    strength = jax.random.uniform(sub_keys[2], (TOKENS, TOP_K), jnp.float32, 0.6, 1.1) * math.log(NUM_EXPERTS)
    picked = (top_ids[:, :, None] == jnp.arange(NUM_EXPERTS)[None, None, :]).astype(jnp.float32)
    coeffs = jnp.einsum('tk,tke->te', strength, picked)
    noise_val = jax.random.normal(sub_keys[3], (TOKENS, MODEL_DIM), jnp.float32)
    x_in = (noise_val + jnp.dot(coeffs, w_router.astype(jnp.float32).T)).astype(jnp.bfloat16)
    dy_in = jax.random.normal(sub_keys[4], (TOKENS, MODEL_DIM), jnp.float32).astype(jnp.bfloat16)
    w_gate = (jax.random.normal(sub_keys[5], (NUM_EXPERTS, MODEL_DIM, EXPERT_FF), jnp.float32) * MODEL_DIM ** -0.5).astype(jnp.bfloat16)
    w_up = (jax.random.normal(sub_keys[6], (NUM_EXPERTS, MODEL_DIM, EXPERT_FF), jnp.float32) * MODEL_DIM ** -0.5).astype(jnp.bfloat16)
    w_down = (jax.random.normal(sub_keys[7], (NUM_EXPERTS, EXPERT_FF, MODEL_DIM), jnp.float32) * EXPERT_FF ** -0.5).astype(jnp.bfloat16)
    s_gate = (jax.random.normal(sub_keys[8], (MODEL_DIM, SHARED_FF), jnp.float32) * MODEL_DIM ** -0.5).astype(jnp.bfloat16)
    s_up = (jax.random.normal(sub_keys[9], (MODEL_DIM, SHARED_FF), jnp.float32) * MODEL_DIM ** -0.5).astype(jnp.bfloat16)
    s_down = (jax.random.normal(sub_keys[10], (SHARED_FF, MODEL_DIM), jnp.float32) * (0.5 * SHARED_FF ** -0.5)).astype(jnp.bfloat16)
    return {'x_in': x_in, 'dy_in': dy_in, 'top_ids': top_ids, 'w_router': w_router, 'w_gate': w_gate, 'w_up': w_up, 'w_down': w_down, 's_gate': s_gate, 's_up': s_up, 's_down': s_down}


def slot_tables(top_blk):
    flat_ids = top_blk.reshape(-1)
    sort_order = jnp.argsort(flat_ids, stable=True)
    counts = jnp.bincount(flat_ids, length=NUM_EXPERTS)
    starts = jnp.cumsum(counts) - counts
    slot_idx = jnp.arange(SLOT_CAP)
    is_valid = slot_idx[None, :] < counts[:, None]
    assign = sort_order[jnp.minimum(starts[:, None] + slot_idx[None, :], TOK_DEV * TOP_K - 1)]
    inverse = jnp.argsort(sort_order, stable=True)
    slot_pos = flat_ids * SLOT_CAP + inverse - starts[flat_ids]
    return assign, is_valid, slot_pos


def silu_grads(d_hidden, gate_pre, up_pre):
    sig_gate = jax.nn.sigmoid(gate_pre)
    silu_gate = gate_pre * sig_gate
    d_gate = (d_hidden * up_pre * sig_gate * (1.0 + gate_pre * (1.0 - sig_gate))).astype(jnp.bfloat16)
    d_up = (d_hidden * silu_gate).astype(jnp.bfloat16)
    return d_gate, d_up


def reference(x_in, dy_in, top_ids, w_router, w_gate, w_up, w_down, s_gate, s_up, s_down):
    logits = jnp.dot(x_in, w_router, preferred_element_type=jnp.float32)
    router_prob = jax.nn.softmax(logits, axis=-1)
    picked = (top_ids[:, :, None] == jnp.arange(NUM_EXPERTS)[None, None, :]).astype(jnp.float32)
    gate_vals = jnp.einsum('tke,te->tk', picked, router_prob)
    gate_f32 = w_gate.astype(jnp.float32)
    up_f32 = w_up.astype(jnp.float32)
    down_f32 = w_down.astype(jnp.float32)

    def block_step(acc_grads, blk_data):
        x_blk, dy_blk, top_blk, gate_blk = blk_data
        assign, is_valid, slot_pos = slot_tables(top_blk)
        src_tok = assign // TOP_K
        rows_x = jnp.where(is_valid[:, :, None], x_blk[src_tok], 0).astype(jnp.float32)
        slot_gate = jnp.where(is_valid, gate_blk.reshape(-1)[assign], 0.0)
        rows_g = (slot_gate[:, :, None] * dy_blk[src_tok].astype(jnp.float32)).astype(jnp.bfloat16).astype(jnp.float32)
        gate_pre = jnp.einsum('ecd,edf->ecf', rows_x, gate_f32)
        up_pre = jnp.einsum('ecd,edf->ecf', rows_x, up_f32)
        hidden = (jax.nn.silu(gate_pre) * up_pre).astype(jnp.bfloat16).astype(jnp.float32)
        out_rows = jnp.einsum('ecf,efd->ecd', hidden, down_f32).astype(jnp.bfloat16)
        d_hidden = jnp.einsum('ecd,efd->ecf', rows_g, down_f32)
        d_gate, d_up = silu_grads(d_hidden, gate_pre, up_pre)
        d_gate = d_gate.astype(jnp.float32)
        d_up = d_up.astype(jnp.float32)
        gw_gate = acc_grads[0] + jnp.einsum('ecd,ecf->edf', rows_x, d_gate)
        gw_up = acc_grads[1] + jnp.einsum('ecd,ecf->edf', rows_x, d_up)
        gw_down = acc_grads[2] + jnp.einsum('ecf,ecd->efd', hidden, rows_g)
        dx_rows = (jnp.einsum('ecf,edf->ecd', d_gate, gate_f32) + jnp.einsum('ecf,edf->ecd', d_up, up_f32)).astype(jnp.bfloat16)
        out_tok = out_rows.reshape(-1, MODEL_DIM)[slot_pos].reshape(TOK_DEV, TOP_K, MODEL_DIM).astype(jnp.float32)
        dx_tok = dx_rows.reshape(-1, MODEL_DIM)[slot_pos].reshape(TOK_DEV, TOP_K, MODEL_DIM).astype(jnp.float32)
        routed = jnp.sum(gate_blk[:, :, None] * out_tok, axis=1)
        gate_grad = jnp.einsum('td,tkd->tk', dy_blk.astype(jnp.float32), out_tok)
        dx_routed = jnp.sum(dx_tok, axis=1)
        return (gw_gate, gw_up, gw_down), (routed, gate_grad, dx_routed)

    zero_gate = jnp.zeros((NUM_EXPERTS, MODEL_DIM, EXPERT_FF), jnp.float32)
    zero_down = jnp.zeros((NUM_EXPERTS, EXPERT_FF, MODEL_DIM), jnp.float32)
    blk_inputs = (x_in.reshape(NUM_BLOCKS, TOK_DEV, MODEL_DIM), dy_in.reshape(NUM_BLOCKS, TOK_DEV, MODEL_DIM), top_ids.reshape(NUM_BLOCKS, TOK_DEV, TOP_K), gate_vals.reshape(NUM_BLOCKS, TOK_DEV, TOP_K))
    grads_out, per_blk = lax.scan(block_step, (zero_gate, zero_gate, zero_down), blk_inputs)
    routed = per_blk[0].reshape(TOKENS, MODEL_DIM)
    gate_grad = per_blk[1].reshape(TOKENS, TOP_K)
    dx_routed = per_blk[2].reshape(TOKENS, MODEL_DIM)

    sg_pre = jnp.dot(x_in, s_gate, preferred_element_type=jnp.float32)
    su_pre = jnp.dot(x_in, s_up, preferred_element_type=jnp.float32)
    s_hidden = (jax.nn.silu(sg_pre) * su_pre).astype(jnp.bfloat16)
    s_out = jnp.dot(s_hidden, s_down, preferred_element_type=jnp.float32)
    y_out = (routed + s_out).astype(jnp.bfloat16)

    d_prob = jnp.einsum('tke,tk->te', picked, gate_grad)
    d_logit = (router_prob * (d_prob - jnp.sum(router_prob * d_prob, axis=-1, keepdims=True))).astype(jnp.bfloat16)
    dw_router = jnp.dot(x_in.T, d_logit, preferred_element_type=jnp.float32)
    dx_router = jnp.dot(d_logit, w_router.T, preferred_element_type=jnp.float32)
    ds_hidden = jnp.dot(dy_in, s_down.T, preferred_element_type=jnp.float32)
    ds_gate_pre, ds_up_pre = silu_grads(ds_hidden, sg_pre, su_pre)
    ds_down = jnp.dot(s_hidden.T, dy_in, preferred_element_type=jnp.float32)
    ds_gate = jnp.dot(x_in.T, ds_gate_pre, preferred_element_type=jnp.float32)
    ds_up = jnp.dot(x_in.T, ds_up_pre, preferred_element_type=jnp.float32)
    dx_shared = jnp.dot(ds_gate_pre, s_gate.T, preferred_element_type=jnp.float32) + jnp.dot(ds_up_pre, s_up.T, preferred_element_type=jnp.float32)
    dx_out = (dx_routed + dx_shared + dx_router).astype(jnp.bfloat16)
    return (y_out, dx_out, dw_router, grads_out[0], grads_out[1], grads_out[2], ds_gate, ds_up, ds_down)
```

```python
import jax
import jax.numpy as jnp
from jax import lax
from jax.sharding import PartitionSpec as P

CHUNKS = 4


def silu_grads(d_hidden, gate_pre, up_pre):
    sig_gate = jax.nn.sigmoid(gate_pre)
    silu_gate = gate_pre * sig_gate
    d_gate = (d_hidden * up_pre * sig_gate * (1.0 + gate_pre * (1.0 - sig_gate))).astype(jnp.bfloat16)
    d_up = (d_hidden * silu_gate).astype(jnp.bfloat16)
    return d_gate, d_up


def ein(spec, a, b):
    return jnp.einsum(spec, a, b, preferred_element_type=jnp.float32)


def solution(mesh):
    all_axes = ('dp', 'ep')
    dp, ep = mesh.shape['dp'], mesh.shape['ep']
    row_spec = P(all_axes, None)
    expert_spec = P('ep', 'dp', None)

    def gather_all(v):
        v = lax.all_gather(v, 'dp', axis=0, tiled=False)
        v = lax.all_gather(v, 'ep', axis=0, tiled=False)
        return v.reshape((dp * ep,) + v.shape[2:])

    def scatter_sum(v):
        v = v.reshape((ep, dp) + v.shape[1:])
        v = lax.psum_scatter(v, 'ep', scatter_dimension=0, tiled=False)
        return lax.psum_scatter(v, 'dp', scatter_dimension=0, tiled=False)

    def xperm(v, m):
        return lax.ppermute(v, 'dp', [(i, i ^ m) for i in range(dp)])

    def local_step(x_loc, dy_loc, top_loc, wr_loc, wg_loc, wu_loc, wd_loc, sg_loc, su_loc, sd_loc):
        d = lax.axis_index('dp')
        h = lax.axis_index('ep')
        tok_count, top_k = top_loc.shape
        model_dim = x_loc.shape[1]
        num_experts = wr_loc.shape[1]
        own = num_experts // (dp * ep)
        slot_cap = 2 * tok_count * top_k // num_experts
        nblk = dp * ep
        per = own // CHUNKS
        base = (h * dp + d) * own

        w_router = lax.all_gather(wr_loc, all_axes, axis=0, tiled=True)
        top_all = gather_all(top_loc)
        x_all = gather_all(x_loc)
        dy_all = gather_all(dy_loc)

        logits = jnp.dot(x_loc, w_router, preferred_element_type=jnp.float32)
        router_prob = jax.nn.softmax(logits, axis=-1)
        p_all = gather_all(router_prob)

        def exchange_weight(w, ci):
            k, n = w.shape[1], w.shape[2]
            wc = w.reshape(dp, own, k, n)[:, ci * per:(ci + 1) * per]
            full = jnp.zeros((per, dp, k, n), w.dtype)
            for m in range(dp):
                part = lax.dynamic_index_in_dim(wc, d ^ m, 0, keepdims=False)
                if m:
                    part = xperm(part, m)
                full = lax.dynamic_update_slice(full, part[:, None], (0, d ^ m, 0, 0))
            return full.reshape(per, dp * k, n)

        def return_grad(buf, g, ci):
            k, n = g.shape[1] // dp, g.shape[2]
            gr = g.reshape(per, dp, k, n)
            for m in range(dp):
                part = lax.dynamic_index_in_dim(gr, d ^ m, 1, keepdims=False)
                if m:
                    part = xperm(part, m)
                buf = lax.dynamic_update_slice(buf, part[None], (d ^ m, ci * per, 0, 0))
            return buf

        ids = base + jnp.arange(own)
        sel = jnp.any(top_all[:, :, :, None] == ids, axis=2)
        tri = (jnp.arange(tok_count)[:, None] > jnp.arange(tok_count)[None, :]).astype(jnp.bfloat16)
        rank = ein('tu,suj->sjt', tri, sel.astype(jnp.bfloat16))
        selt = jnp.swapaxes(sel, 1, 2)
        rank = jnp.where(selt, rank, -1.0)
        gates = jnp.swapaxes(lax.dynamic_slice_in_dim(p_all, base, own, axis=2), 1, 2)

        slot_id = jnp.arange(slot_cap, dtype=jnp.float32)
        gw = [jnp.zeros((dp, own) + w.shape[1:], jnp.float32) for w in (wg_loc, wu_loc, wd_loc)]
        parts, dx_list, hots, dps = [], [], [], []
        for ci in range(CHUNKS):
            w_gate = exchange_weight(wg_loc, ci)
            w_up = exchange_weight(wu_loc, ci)
            w_down = exchange_weight(wd_loc, ci)
            rk = rank[:, ci * per:(ci + 1) * per]
            hit = rk[:, :, None, :] == slot_id[None, None, :, None]
            hot = hit.astype(jnp.bfloat16)
            g_slot = jnp.sum(jnp.where(hit, gates[:, ci * per:(ci + 1) * per, None, :], 0.0), axis=-1)
            xs = ein('sjit,std->jsid', hot, x_all).astype(jnp.bfloat16)
            dys = ein('sjit,std->jsid', hot, dy_all).astype(jnp.bfloat16)
            gs = jnp.swapaxes(g_slot, 0, 1)[..., None]
            rs = (gs * dys.astype(jnp.float32)).astype(jnp.bfloat16)
            gate_pre = ein('jsid,jdf->jsif', xs, w_gate)
            up_pre = ein('jsid,jdf->jsif', xs, w_up)
            hidden = (jax.nn.silu(gate_pre) * up_pre).astype(jnp.bfloat16)
            out = ein('jsif,jfd->jsid', hidden, w_down).astype(jnp.bfloat16)
            outf = out.astype(jnp.float32)
            q = jnp.sum(outf * dys.astype(jnp.float32), axis=-1)
            z = gs * outf
            z1 = lax.reduce_precision(z, 8, 7)
            z2 = lax.reduce_precision(z - z1, 8, 7)
            z3 = z - z1 - z2
            parts.append(jnp.stack([z1.astype(jnp.bfloat16), z2.astype(jnp.bfloat16), z3.astype(jnp.bfloat16)]))
            dc = ein('jsid,jfd->jsif', rs, w_down)
            a, b = silu_grads(dc, gate_pre, up_pre)
            g_down = ein('jsif,jsid->jfd', hidden, rs)
            g_gate = ein('jsid,jsif->jdf', xs, a)
            g_up = ein('jsid,jsif->jdf', xs, b)
            gw[0] = return_grad(gw[0], g_gate, ci)
            gw[1] = return_grad(gw[1], g_up, ci)
            gw[2] = return_grad(gw[2], g_down, ci)
            dxr = (ein('jsif,jdf->jsid', a, w_gate) + ein('jsif,jdf->jsid', b, w_up)).astype(jnp.bfloat16)
            dx_list.append(dxr)
            hots.append(hot)
            qs = jnp.swapaxes(q, 0, 1)
            dps.append(jnp.sum(jnp.where(hit, qs[..., None], 0.0), axis=2))
        hot = jnp.concatenate(hots, axis=1)
        dxc = jnp.concatenate(dx_list, axis=0)
        zc = jnp.concatenate(parts, axis=1)
        y_part = ein('sjit,jsid->std', hot, zc[0]) + ein('sjit,jsid->std', hot, zc[1]) + ein('sjit,jsid->std', hot, zc[2])
        dx_part = ein('sjit,jsid->std', hot, dxc)
        dp_part = jnp.swapaxes(jnp.concatenate(dps, axis=1), 1, 2)
        dp_full = lax.dynamic_update_slice(jnp.zeros((nblk, tok_count, num_experts), jnp.float32), dp_part, (0, 0, base))
        d_prob = scatter_sum(dp_full)
        routed = scatter_sum(y_part)
        dx_routed = scatter_sum(dx_part)

        s_gate = lax.all_gather(sg_loc, all_axes, axis=0, tiled=True)
        s_up = lax.all_gather(su_loc, all_axes, axis=0, tiled=True)
        s_down = lax.all_gather(sd_loc, all_axes, axis=0, tiled=True)
        sg_pre = jnp.dot(x_loc, s_gate, preferred_element_type=jnp.float32)
        su_pre = jnp.dot(x_loc, s_up, preferred_element_type=jnp.float32)
        s_hidden = (jax.nn.silu(sg_pre) * su_pre).astype(jnp.bfloat16)
        s_out = jnp.dot(s_hidden, s_down, preferred_element_type=jnp.float32)
        ds_hidden = ein('td,fd->tf', dy_loc, s_down)
        ds_gate_pre, ds_up_pre = silu_grads(ds_hidden, sg_pre, su_pre)
        gs_down = ein('tf,td->fd', s_hidden, dy_loc)
        gs_gate = ein('td,tf->df', x_loc, ds_gate_pre)
        gs_up = ein('td,tf->df', x_loc, ds_up_pre)
        dx_shared = ein('tf,df->td', ds_gate_pre, s_gate) + ein('tf,df->td', ds_up_pre, s_up)

        y_loc = (routed + s_out).astype(jnp.bfloat16)
        d_logit = (router_prob * (d_prob - jnp.sum(router_prob * d_prob, axis=-1, keepdims=True))).astype(jnp.bfloat16)
        gw_router = ein('td,te->de', x_loc, d_logit)
        dx_router = ein('te,de->td', d_logit, w_router)
        dx_loc = (dx_routed + dx_shared + dx_router).astype(jnp.bfloat16)
        return (y_loc, dx_loc,
                lax.psum_scatter(gw_router, all_axes, scatter_dimension=0, tiled=True),
                gw[0].reshape(wg_loc.shape), gw[1].reshape(wu_loc.shape), gw[2].reshape(wd_loc.shape),
                lax.psum_scatter(gs_gate, all_axes, scatter_dimension=0, tiled=True),
                lax.psum_scatter(gs_up, all_axes, scatter_dimension=0, tiled=True),
                lax.psum_scatter(gs_down, all_axes, scatter_dimension=0, tiled=True))

    return jax.shard_map(local_step, mesh=mesh,
                         in_specs=(row_spec, row_spec, row_spec, row_spec, expert_spec, expert_spec, expert_spec, row_spec, row_spec, row_spec),
                         out_specs=(row_spec, row_spec, row_spec, expert_spec, expert_spec, expert_spec, row_spec, row_spec, row_spec),
                         check_vma=False)
```
